32 devices in a mesh: energy: 16 (over z, x, core), seg: 2 (over y).
Axes of the slice: x: 2, y: 2, z: 4, core: 2. Of those that a mesh axis runs over, the one named last changes fastest.
Arguments:
- onsite: float32 [2, 384, 384], P('seg'), may hold values from -3 to 8
- coupling: float32 [2, 384, 384], P('seg'), may hold values from -2 to 2
- phonon: float32 [2, 384, 384], P('seg'), may hold values from -1 to 1
- levels: float32 [16], P('energy'), may hold values from 0.5 to 2
- offsets: int32 [2], replicated, may hold values from 1 to 15
Outputs:
- green_fn: float32 [16, 2, 384, 384], P('energy', 'seg')
- self_energy: float32 [16, 2, 384, 384], P('energy', 'seg')
The draws below stay inside these ranges and needn't reach their ends.
All inputs are finite; a program needn't handle non-finite values.
Results may differ from the reference program's by a relative error of at most 0.0001.
Values sent between devices are 32-bit elements; how exact they have to be, the bound alone decides.
No kernel may reach another device: no remote copies, remote signals or barrier semaphores. Data moves between devices by JAX's collectives and lax.ppermute only.
A program may use at most 64 MiB of HBM per device.

```python
import math
import jax
import jax.numpy as jnp
from jax import lax

NB = 384
NS = 4
BORN = 2
NE = 16
SEGS = 2


def draw_onsite(key, part):
    first_key, second_key = jax.random.split(jax.random.fold_in(key, 11))
    identity = jnp.eye(NB, dtype=jnp.float32)
    diagonal_part = jax.random.uniform(first_key, (SEGS, NB, 1), jnp.float32, 3.0, 5.0)
    scatter_part = jnp.clip(jax.random.normal(second_key, (SEGS, NB, NB), jnp.float32), -6.0, 6.0) * (2.6 / NB ** 0.5)
    return scatter_part + diagonal_part * identity


def draw_coupling(key, part):
    inner_key = jax.random.fold_in(key, 23)
    values = jnp.clip(jax.random.normal(inner_key, (SEGS, NB, NB), jnp.float32), -6.0, 6.0) * (1.2 / NB ** 0.5)
    return values


def draw_phonon(key, part):
    inner_key = jax.random.fold_in(key, 37)
    values = jnp.clip(jax.random.normal(inner_key, (SEGS, NB, NB), jnp.float32), -6.0, 6.0) * (0.7 / NB ** 0.5)
    return values


def block_levels(rng, dims, cuts, least, top_value):
    factor_of, own = 1.0, jax.random.fold_in(rng, 6)
    for axis_at, parts in cuts:
        draws = jnp.exp(jax.random.uniform(jax.random.fold_in(own, axis_at), (parts,), jnp.float32, least / len(cuts), top_value / len(cuts)))
        factor_of = factor_of * jnp.repeat(draws, dims[axis_at] // parts).reshape([-1 if axis == axis_at else 1 for axis in range(len(dims))])
    return factor_of


def setup_inputs(seed: int = 0) -> dict:
    key_list = jax.random.split(jax.random.key(seed), 6)
    onsite = draw_onsite(jax.random.fold_in(key_list[5], 71), 0)
    coupling = draw_coupling(jax.random.fold_in(key_list[5], 71), 0)
    phonon = draw_phonon(jax.random.fold_in(key_list[5], 71), 0)
    levels = jnp.clip(jnp.exp(math.log(2.0) - 1.3862944 * jax.random.uniform(key_list[3], (NE,), jnp.float32) ** block_levels(key_list[3], (NE,), ((0, 16),), -0.2, 0.2)), 0.5, 2.0)
    offsets = jax.random.randint(key_list[4], (2,), 1, 16).astype(jnp.int32)
    return {"onsite": onsite, "coupling": coupling, "phonon": phonon, "levels": levels, "offsets": offsets}


def product(left_block, right_block):
    return jnp.matmul(left_block, right_block, precision=lax.Precision.HIGHEST)


def transpose(matrix):
    return jnp.swapaxes(matrix, -1, -2)


def invert(matrix):
    order_size = matrix.shape[-1]
    identity = jnp.eye(order_size, dtype=jnp.float32)
    approx = identity / jnp.diagonal(matrix, axis1=-2, axis2=-1)[..., None, :]
    for sweep_index in range(NS):
        approx = product(approx, 2.0 * identity - product(matrix, approx))
    return approx


def dyson_sweep(onsite, coupling, levels, self_energy):
    seg_total = onsite.shape[0]
    identity = jnp.eye(onsite.shape[-1], dtype=jnp.float32)
    lead_term = product(coupling[0], transpose(coupling[0])) * 0.25
    left_list = []
    for segment in range(seg_total):
        matrix = onsite[segment] + levels[:, None, None] * identity + self_energy[:, segment]
        if segment == 0:
            inner_term = lead_term
        else:
            inner_term = product(product(coupling[segment], left_list[-1]), transpose(coupling[segment]))
        left_list.append(invert(matrix - inner_term))
    full_blocks = [None] * seg_total
    full_blocks[seg_total - 1] = left_list[seg_total - 1]
    for segment in range(seg_total - 2, -1, -1):
        next_coupling = coupling[segment + 1]
        weight_in = product(product(transpose(next_coupling), full_blocks[segment + 1]), next_coupling)
        left_block = left_list[segment]
        full_blocks[segment] = left_block + product(product(left_block, weight_in), left_block)
    return jnp.stack(full_blocks, axis=1)


def shifted(field, amount):
    count_energy = field.shape[0]
    positions = jnp.arange(count_energy, dtype=jnp.int32)
    source = (positions - amount).astype(jnp.int32)
    inside = ((source >= 0) & (source < count_energy)).astype(jnp.float32)
    gathered = jnp.take(field, jnp.clip(source, 0, count_energy - 1).astype(jnp.int32), axis=0)
    return gathered * inside[:, None, None, None]


def phonon_term(green_fn, phonon, offsets):
    combined = shifted(green_fn, offsets[0]) + shifted(green_fn, offsets[1])
    combined = combined + shifted(green_fn, -offsets[0]) + shifted(green_fn, -offsets[1])
    return product(product(phonon[None], combined), transpose(phonon)[None])


def reference(onsite, coupling, phonon, levels, offsets):
    self_energy = jnp.zeros((levels.shape[0],) + onsite.shape, dtype=jnp.float32)
    green_fn = self_energy
    for round_index in range(BORN):
        green_fn = dyson_sweep(onsite, coupling, levels, self_energy)
        if round_index < BORN - 1:
            self_energy = phonon_term(green_fn, phonon, offsets)
    return green_fn, self_energy
```

```python
import functools

import jax
import jax.numpy as jnp
from jax import lax
from jax.experimental import pallas as pl
from jax.experimental.pallas import tpu as pltpu
from jax.sharding import PartitionSpec as P

NS = 4
VMEM_BYTES = 62 * 2**20
F32, BF16 = jnp.float32, jnp.bfloat16


def split(x):
    high = x.astype(BF16)
    return high, (x - high.astype(F32)).astype(BF16)


def product(a, b):
    left = jnp.concatenate([a[0], a[0], a[1]], axis=1)
    right = jnp.concatenate([b[0], b[1], b[0]], axis=0)
    return jnp.dot(left, right, preferred_element_type=F32)


def beside(a, b):
    return tuple(jnp.concatenate([x, y], axis=1) for x, y in zip(a, b))


def joined(a):
    return a[0].astype(F32) + a[1].astype(F32)


def eye_mask(n):
    return lax.broadcasted_iota(jnp.int32, (n, n), 0) == lax.broadcasted_iota(jnp.int32, (n, n), 1)


def diagonal(x, axis):
    n, step = x.shape[0], 128
    mask = eye_mask(step)
    blocks = [
        jnp.sum(jnp.where(mask, x[i : i + step, i : i + step], 0.0), axis=axis, keepdims=True)
        for i in range(0, n, step)
    ]
    return jnp.concatenate(blocks, axis=1 - axis)


def over(low, high, body):
    if high - low == 1:
        body(low)
    elif high > low:
        lax.fori_loop(low, high, lambda s, _: (body(s), None)[1], None)


class Pair:
    def __init__(self, ref):
        self.ref = ref

    def put(self, index, value):
        self.ref[(*index, 0)], self.ref[(*index, 1)] = split(value)

    def get(self, *index):
        return self.ref[(*index, 0)], self.ref[(*index, 1)]


def invert(matrices, power, poly, row_scale, store):
    lanes = range(len(matrices))
    for i in lanes:
        x = matrices[i]()
        n = x.shape[0]
        identity = jnp.where(eye_mask(n), 1.0, 0.0)
        residual = identity - x * (1.0 / diagonal(x, 0))
        row_scale[i] = jnp.broadcast_to(1.0 / diagonal(x, 1), (n, 128))
        power.put((i,), residual)
        poly.put((i,), identity + residual)
    for i in lanes:
        e = power.get(i)
        power.put((i,), product(e, e))
    for step in range(2, NS):
        for i in lanes:
            e, p = power.get(i), poly.get(i)
            both = product(e, beside(e, p))
            n = both.shape[0]
            power.put((i,), both[:, :n])
            poly.put((i,), both[:, n:] + joined(p))
    for i in lanes:
        p = poly.get(i)
        total = product(power.get(i), p) + joined(p)
        n = total.shape[0]
        store(i, total * jnp.concatenate([row_scale[i]] * (n // 128), axis=1))


def sweep(lanes, segs, matrix, coupling, coupling_t, left, left_pair, green, work, power, poly, row_scale, emit, wanted=None):
    right, outer = work

    def forward(s):
        def load(i):
            x = matrix(s, i)
            if not (isinstance(s, int) and s == 0):
                x = x - left[s, i]
            return x

        def store(i, value):
            left[s, i] = value
            left_pair.put((i,), value)

        invert([functools.partial(load, i) for i in range(lanes)], power, poly, row_scale, store)

    def hand_over(s):
        for i in range(lanes):
            outer.put((s, i), product(left_pair.get(i), coupling_t.get(s + 1)))
        for i in range(lanes):
            both = product(coupling.get(s + 1), beside(left_pair.get(i), outer.get(s, i)))
            n = both.shape[0]
            right.put((s, i), both[:, :n])
            left[s + 1, i] = both[:, n:]

    forward(0)

    def advance(s):
        hand_over(s - 1)
        forward(s)

    over(1, segs, advance)
    for i in range(lanes):
        green.put((i,), left[segs - 1, i])
        emit(segs - 1, i, left[segs - 1, i])

    def backward(turn):
        s = segs - 1 - turn

        def settle():
            for i in range(lanes):
                green.put((i,), product(green.get(i), right.get(s, i)))
            for i in range(lanes):
                value = left[s, i] + product(outer.get(s, i), green.get(i))
                green.put((i,), value)
                emit(s, i, value)

        if wanted is None:
            settle()
        else:
            pl.when(wanted(s))(settle)

    over(1, segs, backward)


def place(target, own, received, at, slot, sems):
    seg, segs, parity = at
    half = target.shape[1] // 2
    copies = [(own, target.at[seg])]
    for d in range(1, segs):
        source = lax.rem(seg - d + segs, segs)
        for block, which in zip(received[d - 1], (parity, 1 - parity)):
            rows = pl.ds(pl.multiple_of(which * half, half), half)
            copies.append((block.at[slot], target.at[source, rows, :]))
    copies = [pltpu.make_async_copy(*ends, sems.at[k]) for k, ends in enumerate(copies)]
    for copy in copies:
        copy.start()
    return copies


def first_round(segs, count, lanes, index, levels, *refs):
    own_matrix, own_coupling = refs[:2]
    received = [(refs[2 + 2 * k], refs[3 + 2 * k]) for k in range(segs - 1)]
    combined, onsite, coupling, coupling_t, stage, left, left_pair, green, right, outer, power, poly, row_scale, sems, chosen = refs[2 * segs :]
    energy, seg = index[0], index[1]
    at = (seg, segs, lax.rem(energy, 2))
    copies = place(onsite, own_matrix, received, at, 0, sems.at[0])
    copies += place(stage, own_coupling, received, at, 1, sems.at[1])
    for copy in copies:
        copy.wait()
    coupling, coupling_t = Pair(coupling), Pair(coupling_t)

    def prepare(s):
        value = stage[s]
        coupling.put((s,), value)
        coupling_t.put((s,), value.T)

    over(1, segs, prepare)

    total = jnp.int32(0)
    for sign in (-1, 1):
        for k in range(2):
            source = energy + sign * index[2 + k]
            inside = (source >= 0) & (source < count)
            chosen[total] = levels[jnp.clip(source, 0, count - 1)]
            total = total + inside.astype(jnp.int32)
    combined[...] = jnp.zeros_like(combined)
    n = onsite.shape[1]

    def turn(k, _):
        active = [k * lanes + i < total for i in range(lanes)]
        shift = [chosen[jnp.where(active[i], k * lanes + i, k * lanes)] for i in range(lanes)]

        def matrix(s, i):
            return onsite[s] + jnp.where(eye_mask(n), shift[i], 0.0)

        def emit(s, i, value):
            if i == 0:
                combined[s] += value
            else:
                combined[s] += jnp.where(active[i], value, 0.0)

        sweep(
            lanes, segs, matrix, coupling, coupling_t, left, Pair(left_pair), Pair(green),
            (Pair(right), Pair(outer)), Pair(power), Pair(poly), row_scale, emit,
        )

    lax.fori_loop(0, pl.cdiv(total, lanes), turn, None)


def second_round(segs, index, level, *refs):
    own_matrix, own_coupling, own_phonon = refs[:3]
    received = [(refs[3 + 2 * k], refs[4 + 2 * k]) for k in range(segs - 1)]
    received_phonon = [(refs[1 + 2 * segs + 2 * k], refs[2 + 2 * segs + 2 * k]) for k in range(segs - 1)]
    rest = refs[4 * segs - 1 :]
    combined, green_out, energy_out = rest[:3]
    onsite, coupling, coupling_t, stage, left, left_pair, green, right, outer, power, poly, row_scale, sems, phonon = rest[3:]
    energy, seg = index[0], index[1]
    at = (seg, segs, lax.rem(energy, 2))
    power, poly = Pair(power), Pair(poly)
    copies = place(onsite, own_matrix, received, at, 0, sems.at[0])
    copies += place(stage, own_coupling, received, at, 1, sems.at[1])
    copies += place(phonon, own_phonon, received_phonon, at, 0, sems.at[2])
    for copy in copies:
        copy.wait()
    coupling, coupling_t = Pair(coupling), Pair(coupling_t)

    def prepare(s):
        value = stage[s]
        coupling.put((s,), value)
        coupling_t.put((s,), value.T)

    over(1, segs, prepare)
    n = onsite.shape[1]

    def scatter(s):
        value = phonon[s]
        poly.put((0,), combined[s])
        power.put((0,), value)
        inner = product(power.get(0), poly.get(0))
        power.put((0,), inner)
        poly.put((0,), value.T)
        stage[s] = product(power.get(0), poly.get(0))

    for s in range(segs):
        scatter(s)
    energy_out[...] = stage[seg]

    def matrix(s, i):
        return onsite[s] + jnp.where(eye_mask(n), level[0], 0.0) + stage[s]

    def emit(s, i, value):
        @pl.when(seg == s)
        def _():
            green_out[...] = value

    sweep(
        1, segs, matrix, coupling, coupling_t, left, Pair(left_pair), Pair(green),
        (Pair(right), Pair(outer)), power, poly, row_scale, emit, lambda s: seg <= s,
    )


def scratch(segs, n, lanes):
    def pair(*lead):
        return pltpu.VMEM((*lead, 2, n, n), BF16)

    def full(*lead):
        return pltpu.VMEM((*lead, n, n), F32)

    return [
        full(segs), pair(segs), pair(segs), full(segs), full(segs, lanes), pair(lanes), pair(lanes),
        pair(segs, lanes), pair(segs, lanes), pair(lanes), pair(lanes), pltpu.VMEM((lanes, n, 128), F32),
        pltpu.SemaphoreType.DMA((3, 2 * segs)),
    ]


def swapped(block, axis, distance):
    size = lax.axis_size(axis)
    return lax.ppermute(block, axis, [(i, (i + distance) % size) for i in range(size)])


def partner(block, axis, bit):
    size = lax.axis_size(axis)
    return lax.ppermute(block, axis, [(i, i ^ bit) for i in range(size)])


def every_level(levels):
    size, bit = lax.axis_size("energy"), 1
    place_of = lax.axis_index("energy")
    while bit < size:
        other = partner(levels, "energy", bit)
        low = place_of & bit == 0
        levels = jnp.where(low, jnp.concatenate([levels, other]), jnp.concatenate([other, levels]))
        bit *= 2
    return levels


def from_others(stack):
    half = stack.shape[1] // 2
    parity = lax.axis_index("energy") % 2
    mine = lax.dynamic_slice_in_dim(stack, parity * half, half, 1)
    pieces = []
    for d in range(1, lax.axis_size("seg")):
        same = swapped(mine, "seg", d)
        pieces += [same, partner(same, "energy", 1)]
    return pieces


def shards(onsite, coupling, phonon, levels, offsets):
    segs, count = lax.axis_size("seg"), lax.axis_size("energy")
    n = onsite.shape[-1]
    energy, seg = lax.axis_index("energy"), lax.axis_index("seg")
    coupling, phonon = coupling[0], phonon[0]
    lead = jnp.matmul(coupling, coupling.T, precision=lax.Precision.HIGHEST) * 0.25
    matrix = onsite[0] - jnp.where(seg == 0, lead, 0.0)
    received = from_others(jnp.stack([matrix, coupling]))
    all_levels = every_level(levels)
    received_phonon = from_others(lax.optimization_barrier((phonon[None], received[-1]))[0])
    index = jnp.concatenate([jnp.stack([energy, seg]).astype(jnp.int32), offsets])
    smem, vmem, where = (pl.BlockSpec(memory_space=m) for m in (pltpu.SMEM, pltpu.VMEM, pl.ANY))
    lanes = 2 if (segs * 13 + 8) * 4 * n * n < VMEM_BYTES else 1
    params = pltpu.CompilerParams(vmem_limit_bytes=VMEM_BYTES)
    combined = pl.pallas_call(
        functools.partial(first_round, segs, count, lanes),
        out_shape=jax.ShapeDtypeStruct((segs, n, n), F32),
        in_specs=[smem, smem] + [where] * (2 * segs),
        out_specs=vmem,
        scratch_shapes=scratch(segs, n, lanes) + [pltpu.SMEM((8,), F32)],
        compiler_params=params,
        cost_estimate=pl.CostEstimate(flops=200 * n**3, bytes_accessed=8 * n * n, transcendentals=0),
        name="first_round",
    )(index, all_levels, matrix, coupling, *received)
    green, self_energy = pl.pallas_call(
        functools.partial(second_round, segs),
        out_shape=[jax.ShapeDtypeStruct((n, n), F32)] * 2,
        in_specs=[smem, smem] + [where] * (4 * segs - 1) + [vmem],
        out_specs=[vmem, vmem],
        scratch_shapes=scratch(segs, n, 1) + [pltpu.VMEM((segs, n, n), F32)],
        compiler_params=params,
        name="second_round",
    )(index, levels, matrix, coupling, phonon, *received, *received_phonon, combined)
    return green[None, None], self_energy[None, None]


def solution(mesh):
    in_specs = (P("seg", None, None), P("seg", None, None), P("seg", None, None), P("energy"), P())
    out_specs = (P("energy", "seg", None, None), P("energy", "seg", None, None))
    return jax.shard_map(shards, mesh=mesh, in_specs=in_specs, out_specs=out_specs, check_vma=False)
```

```python
import functools
import math

import jax
import jax.numpy as jnp
from jax import lax
from jax.experimental import pallas as pl
from jax.experimental.pallas import tpu as pltpu
from jax.sharding import PartitionSpec as P


NS = 4
TERMS = 4
VMEM_BYTES = 52 * 2**20
SPARE_BYTES = 8 * 2**20
F32, BF16 = jnp.float32, jnp.bfloat16


def split(x):
    high = x.astype(BF16)
    return high, (x - high.astype(F32)).astype(BF16)


def product(a, b):
    left = jnp.concatenate([a[0], a[0], a[1]], axis=1)
    right = jnp.concatenate([b[0], b[1], b[0]], axis=0)
    return jnp.dot(left, right, preferred_element_type=F32)


def beside(a, b):
    return tuple(jnp.concatenate([x, y], axis=1) for x, y in zip(a, b))


def joined(a):
    return a[0].astype(F32) + a[1].astype(F32)


def eye_mask(n):
    return lax.broadcasted_iota(jnp.int32, (n, n), 0) == lax.broadcasted_iota(jnp.int32, (n, n), 1)


def diagonal(x, axis):
    n, step = x.shape[0], 128
    mask = eye_mask(step)
    blocks = [
        jnp.sum(jnp.where(mask, x[i : i + step, i : i + step], 0.0), axis=axis, keepdims=True)
        for i in range(0, n, step)
    ]
    return jnp.concatenate(blocks, axis=1 - axis)


def over(low, high, body):
    if high - low == 1:
        body(low)
    elif high > low:
        lax.fori_loop(low, high, lambda s, _: (body(s), None)[1], None)


class Pair:
    def __init__(self, ref):
        self.ref = ref

    def put(self, index, value):
        self.ref[(*index, 0)], self.ref[(*index, 1)] = split(value)

    def get(self, *index):
        return self.ref[(*index, 0)], self.ref[(*index, 1)]


def invert(matrices, power, poly, row_scale, store):
    lanes = range(len(matrices))
    for i in lanes:
        x = matrices[i]()
        n = x.shape[0]
        identity = jnp.where(eye_mask(n), 1.0, 0.0)
        residual = identity - x * (1.0 / diagonal(x, 0))
        row_scale[i] = jnp.broadcast_to(1.0 / diagonal(x, 1), (n, 128))
        power.put((i,), residual)
        poly.put((i,), identity + residual)
    for i in lanes:
        e = power.get(i)
        power.put((i,), product(e, e))
    for _ in range(2, NS):
        for i in lanes:
            e, p = power.get(i), poly.get(i)
            both = product(e, beside(e, p))
            n = both.shape[0]
            power.put((i,), both[:, :n])
            poly.put((i,), both[:, n:] + joined(p))
    for i in lanes:
        p = poly.get(i)
        total = product(power.get(i), p) + joined(p)
        n = total.shape[0]
        store(i, total * jnp.concatenate([row_scale[i]] * (n // 128), axis=1))


def sweep(lanes, segs, matrix, coupling, coupling_t, left, left_pair, green, work, power, poly, row_scale, emit, wanted=None, given=False):
    right, outer = work

    def forward(s):
        def load(i):
            x = matrix(s, i)
            if not (isinstance(s, int) and s == 0):
                x = x - left[s, i]
            return x

        def store(i, value):
            left[s, i] = value
            left_pair.put((i,), value)

        invert([functools.partial(load, i) for i in range(lanes)], power, poly, row_scale, store)

    def hand_over(s):
        for i in range(lanes):
            outer.put((s, i), product(left_pair.get(i), coupling_t.get(s + 1)))
        for i in range(lanes):
            both = product(coupling.get(s + 1), beside(left_pair.get(i), outer.get(s, i)))
            n = both.shape[0]
            right.put((s, i), both[:, :n])
            left[s + 1, i] = both[:, n:]

    if given:
        for i in range(lanes):
            left_pair.put((i,), left[0, i])
    else:
        forward(0)

    def advance(s):
        hand_over(s - 1)
        forward(s)

    over(1, segs, advance)
    for i in range(lanes):
        green.put((i,), left[segs - 1, i])
        emit(segs - 1, i, left[segs - 1, i])

    def backward(turn):
        s = segs - 1 - turn

        def settle():
            for i in range(lanes):
                green.put((i,), product(green.get(i), right.get(s, i)))
            for i in range(lanes):
                value = left[s, i] + product(outer.get(s, i), green.get(i))
                green.put((i,), value)
                emit(s, i, value)

        if wanted is None:
            settle()
        else:
            pl.when(wanted(s))(settle)

    over(1, segs, backward)


def pieces(target, own, received, at):
    seg, segs, parity = at
    copies = [(own, target.at[seg])]
    for d in range(1, segs):
        source = lax.rem(seg - d + segs, segs)
        copies += parts(received[d - 1], target.at[source], parity)
    return copies


def parts(received, target, parity):
    if len(received) == 1:
        return [(received[0], target)]
    half = target.shape[0] // 2
    return [
        (block, target.at[pl.ds(pl.multiple_of(which * half, half), half), :])
        for block, which in zip(received, (parity, 1 - parity))
    ]


def started(ends, sems):
    copies = [pltpu.make_async_copy(*pair, sems.at[k]) for k, pair in enumerate(ends)]
    for copy in copies:
        copy.start()
    return copies


def wait(copies):
    for copy in copies:
        copy.wait()


def taken(refs, segs, each):
    own, *refs = refs
    return own, [refs[each * k : each * (k + 1)] for k in range(segs - 1)], refs[each * (segs - 1) :]


def choose(index, levels, chosen, count):
    total = jnp.int32(0)
    for sign in (-1, 1):
        for k in range(2):
            source = index[0] + sign * index[2 + k]
            inside = (source >= 0) & (source < count)
            chosen[total] = levels[jnp.clip(source, 0, count - 1)]
            total = total + inside.astype(jnp.int32)
    return total


def in_turns(total, lanes, turn):
    whole = total // lanes
    lax.fori_loop(0, whole, lambda k, _: (turn(k * lanes, lanes), None)[1], None)
    if lanes > 1:
        lax.fori_loop(whole * lanes, total, lambda k, _: (turn(k, 1), None)[1], None)


def first_blocks(segs, count, lanes, index, levels, *refs):
    own, received, (left, onsite, power, poly, row_scale, sems, chosen) = taken(refs, segs, 2)
    seg, parity = index[1], lax.rem(index[0], 2)
    n = onsite.shape[0]

    @pl.when(seg == 0)
    def _():
        wait(started([(own, onsite)], sems))

    for d in range(1, segs):

        @pl.when(seg == d)
        def _():
            wait(started(parts(received[d - 1], onsite, parity), sems))

    total = choose(index, levels, chosen, count)

    def turn(at, width):
        def load(i):
            return onsite[...] + jnp.where(eye_mask(n), chosen[at + i], 0.0)

        def store(i, value):
            left[at + i] = value

        invert([functools.partial(load, i) for i in range(width)], Pair(power), Pair(poly), row_scale, store)

    in_turns(total, lanes, turn)


def prepared(stage, coupling, coupling_t, segs):
    def prepare(s):
        value = stage[s]
        coupling.put((s,), value)
        coupling_t.put((s,), value.T)

    over(1, segs, prepare)


def first_round(segs, count, lanes, index, levels, *refs):
    own_matrix, received_matrix, refs = taken(refs, segs, 2)
    own_coupling, received_coupling, refs = taken(refs, segs, 1)
    first, combined, onsite, coupling, coupling_t, stage, left, left_pair, green, right, outer, power, poly, row_scale, sems, chosen, firsts = refs
    at = (index[1], segs, lax.rem(index[0], 2))
    copies = started(pieces(stage, own_coupling, received_coupling, at), sems.at[0])
    copies += started([(first, firsts)], sems.at[2])
    later = started(pieces(onsite, own_matrix, received_matrix, at), sems.at[1])
    total = choose(index, levels, chosen, count)
    combined[...] = jnp.zeros_like(combined)
    wait(copies)
    coupling, coupling_t = Pair(coupling), Pair(coupling_t)
    prepared(stage, coupling, coupling_t, segs)
    wait(later)
    n = onsite.shape[1]

    def turn(at, width):
        for i in range(width):
            left[0, i] = firsts[at + i]

        def matrix(s, i):
            return onsite[s] + jnp.where(eye_mask(n), chosen[at + i], 0.0)

        def emit(s, i, value):
            combined[s] += value

        sweep(
            width, segs, matrix, coupling, coupling_t, left, Pair(left_pair), Pair(green),
            (Pair(right), Pair(outer)), Pair(power), Pair(poly), row_scale, emit, given=True,
        )

    in_turns(total, lanes, turn)


def second_round(segs, index, level, *refs):
    own_matrix, received_matrix, refs = taken(refs, segs, 2)
    own_coupling, received_coupling, refs = taken(refs, segs, 1)
    own_phonon, received_phonon, refs = taken(refs, segs, 1)
    combined_in, green_out, energy_out, *refs = refs
    onsite, coupling, coupling_t, stage, left, left_pair, green, right, outer, power, poly, row_scale, sems, phonon, combined = refs
    seg = index[1]
    at = (seg, segs, lax.rem(index[0], 2))
    copies = started([(combined_in, combined)], sems.at[3])
    copies += started(pieces(phonon, own_phonon, received_phonon, at), sems.at[2])
    later = started(pieces(onsite, own_matrix, received_matrix, at), sems.at[0])
    later += started(pieces(stage, own_coupling, received_coupling, at), sems.at[1])
    coupling, coupling_t, right, outer = Pair(coupling), Pair(coupling_t), Pair(right), Pair(outer)
    n = onsite.shape[1]
    wait(copies)
    for s in range(segs):
        value = phonon[s]
        coupling.put((s,), value)
        coupling_t.put((s,), value.T)
        right.put((s, 0), combined[s])
    for s in range(segs):
        outer.put((s, 0), product(coupling.get(s), right.get(s, 0)))
    for s in range(segs):
        combined[s] = product(outer.get(s, 0), coupling_t.get(s))
    energy_out[...] = combined[seg]
    wait(later)

    def matrix(s, i):
        return onsite[s] + jnp.where(eye_mask(n), level[0], 0.0) + combined[s]

    def emit(s, i, value):
        @pl.when(seg == s)
        def _():
            green_out[...] = value

    prepared(stage, coupling, coupling_t, segs)
    sweep(
        1, segs, matrix, coupling, coupling_t, left, Pair(left_pair), Pair(green),
        (right, outer), Pair(power), Pair(poly), row_scale, emit, lambda s: seg <= s,
    )


def pair(n, *lead):
    return pltpu.VMEM((*lead, 2, n, n), BF16)


def full(n, *lead):
    return pltpu.VMEM((*lead, n, n), F32)


def workspace(segs, n, lanes):
    return [
        full(n, segs), pair(n, segs), pair(n, segs), full(n, segs), full(n, segs, lanes), pair(n, lanes), pair(n, lanes),
        pair(n, segs, lanes), pair(n, segs, lanes), pair(n, lanes), pair(n, lanes), pltpu.VMEM((lanes, n, 128), F32),
        pltpu.SemaphoreType.DMA((4, 2 * segs)),
    ]


def held(shapes):
    return sum(4 * math.prod(s.shape) for s in shapes if s.dtype == F32) + sum(2 * math.prod(s.shape) for s in shapes if s.dtype == BF16)


def call(body, out_shape, operands, scratch, flops):
    smem, vmem, anywhere = (pl.BlockSpec(memory_space=m) for m in (pltpu.SMEM, pltpu.VMEM, pl.ANY))
    outs = jax.tree.leaves(out_shape)
    return pl.pallas_call(
        body,
        out_shape=out_shape,
        in_specs=[smem, smem] + [anywhere] * (len(operands) - 2),
        out_specs=jax.tree.map(lambda _: vmem, out_shape),
        scratch_shapes=scratch,
        compiler_params=pltpu.CompilerParams(vmem_limit_bytes=held(scratch + outs) + SPARE_BYTES),
        cost_estimate=pl.CostEstimate(flops=flops, bytes_accessed=held(outs), transcendentals=0),
    )(*operands)


def swapped(block, axis, distance):
    size = lax.axis_size(axis)
    return lax.ppermute(block, axis, [(i, (i + distance) % size) for i in range(size)])


def partner(block, axis, bit):
    size = lax.axis_size(axis)
    return lax.ppermute(block, axis, [(i, i ^ bit) for i in range(size)])


def every_level(levels):
    size, bit = lax.axis_size("energy"), 1
    place_of = lax.axis_index("energy")
    while bit < size:
        other = partner(levels, "energy", bit)
        low = place_of & bit == 0
        levels = jnp.where(low, jnp.concatenate([levels, other]), jnp.concatenate([other, levels]))
        bit *= 2
    return levels


def half_of(block):
    half = block.shape[0] // 2
    return lax.dynamic_slice_in_dim(block, lax.axis_index("energy") % 2 * half, half, 0)


def from_others(block):
    received = []
    for d in range(1, lax.axis_size("seg")):
        received.append(swapped(block, "seg", d))
    return received


def with_partner(halves):
    return [part for half in halves for part in (half, partner(half, "energy", 1))]


def shards(onsite, coupling, phonon, levels, offsets):
    return both_rounds(onsite[0], coupling[0], phonon[0], levels, offsets)


def both_rounds(onsite, coupling, phonon, levels, offsets):
    segs, count = lax.axis_size("seg"), lax.axis_size("energy")
    n = onsite.shape[-1]
    energy, seg = lax.axis_index("energy"), lax.axis_index("seg")

    def less_lead(block, rows):
        lead = jnp.matmul(rows, coupling.T, precision=lax.Precision.HIGH) * 0.25
        return block - jnp.where(seg == 0, lead, 0.0)

    matrix_half = less_lead(half_of(onsite), half_of(coupling))
    halves = from_others(matrix_half)
    matrices = with_partner(halves)
    all_levels = every_level(levels)
    matrix = less_lead(onsite, lax.optimization_barrier((coupling, matrix_half))[0])
    couplings = from_others(coupling)
    phonons = from_others(phonon)
    index = jnp.concatenate([jnp.stack([energy, seg]).astype(jnp.int32), offsets])
    lanes = 2 if held(workspace(segs, n, 2)) + segs * 4 * n * n < VMEM_BYTES else 1
    shape = functools.partial(jax.ShapeDtypeStruct, dtype=F32)
    chosen = pltpu.SMEM((2 * TERMS,), jnp.float32)
    first = call(
        functools.partial(first_blocks, segs, count, lanes),
        shape((TERMS, n, n)),
        [index, all_levels, matrix, *matrices],
        [full(n), pair(n, lanes), pair(n, lanes), pltpu.VMEM((lanes, n, 128), F32), pltpu.SemaphoreType.DMA((2,)), chosen],
        12 * n**3 * TERMS * 3,
    )
    combined = call(
        functools.partial(first_round, segs, count, lanes),
        shape((segs, n, n)),
        [index, all_levels, matrix, *matrices, coupling, *couplings, first],
        workspace(segs, n, lanes) + [chosen, full(n, TERMS)],
        22 * n**3 * TERMS * 3 * (segs - 1),
    )
    green, self_energy = call(
        functools.partial(second_round, segs),
        [shape((n, n))] * 2,
        [index, levels, matrix, *matrices, coupling, *couplings, phonon, *phonons, combined],
        workspace(segs, n, 1) + [full(n, segs), full(n, segs)],
        36 * n**3 * 3,
    )
    return green[None, None], self_energy[None, None]


def solution(mesh):
    in_specs = (P("seg", None, None), P("seg", None, None), P("seg", None, None), P("energy"), P())
    out_specs = (P("energy", "seg", None, None), P("energy", "seg", None, None))
    return jax.shard_map(shards, mesh=mesh, in_specs=in_specs, out_specs=out_specs, check_vma=False)
```

```python
import functools
import math

import jax
import jax.numpy as jnp
from jax import lax
from jax.experimental import pallas as pl
from jax.experimental.pallas import tpu as pltpu
from jax.sharding import PartitionSpec as P


NS = 4
TERMS = 4
TAIL = 128
VMEM_BYTES = 52 * 2**20
SPARE_BYTES = 8 * 2**20
F32, BF16 = jnp.float32, jnp.bfloat16


def split(x):
    high = x.astype(BF16)
    return high, (x - high.astype(F32)).astype(BF16)


def product(a, b, alone=False):
    rows = a[0].shape[0]
    cut = rows - TAIL if alone else rows
    order = [(which, lo, hi) for lo, hi in ((0, cut), (cut, rows)) if lo < hi for which in ((0, 0), (0, 1), (1, 0))]
    left = jnp.concatenate([a[i][:, lo:hi] for (i, _), lo, hi in order], axis=1)
    right = jnp.concatenate([b[j][lo:hi] for (_, j), lo, hi in order], axis=0)
    parts = [left[:cut], left[cut:]] if alone else [left]
    parts = [jnp.dot(part, right, preferred_element_type=F32) for part in parts]
    return jnp.concatenate(parts, axis=0) if alone else parts[0]


def beside(a, b):
    return tuple(jnp.concatenate([x, y], axis=1) for x, y in zip(a, b))


def joined(a):
    return a[0].astype(F32) + a[1].astype(F32)


def eye_mask(n):
    return lax.broadcasted_iota(jnp.int32, (n, n), 0) == lax.broadcasted_iota(jnp.int32, (n, n), 1)


def diagonal(x, axis):
    n, step = x.shape[0], 128
    mask = eye_mask(step)
    blocks = [
        jnp.sum(jnp.where(mask, x[i : i + step, i : i + step], 0.0), axis=axis, keepdims=True)
        for i in range(0, n, step)
    ]
    return jnp.concatenate(blocks, axis=1 - axis)


def over(low, high, body):
    if high - low == 1:
        body(low)
    elif high > low:
        lax.fori_loop(low, high, lambda s, _: (body(s), None)[1], None)


class Pair:
    def __init__(self, ref):
        self.ref = ref

    def put(self, index, value):
        self.ref[(*index, 0)], self.ref[(*index, 1)] = split(value)

    def get(self, *index):
        return self.ref[(*index, 0)], self.ref[(*index, 1)]


def invert(matrices, power, poly, row_scale, store):
    lanes = range(len(matrices))
    alone = len(matrices) == 1
    for i in lanes:
        x = matrices[i]()
        n = x.shape[0]
        identity = jnp.where(eye_mask(n), 1.0, 0.0)
        residual = identity - x * (1.0 / diagonal(x, 0))
        row_scale[i] = jnp.broadcast_to(1.0 / diagonal(x, 1), (n, 128))
        power.put((i,), residual)
        poly.put((i,), identity + residual)
    for i in lanes:
        e = power.get(i)
        power.put((i,), product(e, e, alone))
    for _ in range(2, NS):
        for i in lanes:
            e, p = power.get(i), poly.get(i)
            both = product(e, beside(e, p), alone)
            n = both.shape[0]
            power.put((i,), both[:, :n])
            poly.put((i,), both[:, n:] + joined(p))
    for i in lanes:
        p = poly.get(i)
        total = product(power.get(i), p, alone) + joined(p)
        n = total.shape[0]
        store(i, total * jnp.concatenate([row_scale[i]] * (n // 128), axis=1))


def sweep(lanes, segs, matrix, coupling, coupling_t, left, left_pair, green, work, power, poly, row_scale, emit, wanted=None, given=False):
    right, outer = work
    alone = lanes == 1

    def forward(s):
        def load(i):
            x = matrix(s, i)
            if not (isinstance(s, int) and s == 0):
                x = x - left[s, i]
            return x

        def store(i, value):
            left[s, i] = value
            left_pair.put((i,), value)

        invert([functools.partial(load, i) for i in range(lanes)], power, poly, row_scale, store)

    def hand_over(s):
        for i in range(lanes):
            outer.put((s, i), product(left_pair.get(i), coupling_t.get(s + 1), alone))
        for i in range(lanes):
            both = product(coupling.get(s + 1), beside(left_pair.get(i), outer.get(s, i)), alone)
            n = both.shape[0]
            right.put((s, i), both[:, :n])
            left[s + 1, i] = both[:, n:]

    if given:
        for i in range(lanes):
            left_pair.put((i,), left[0, i])
    else:
        forward(0)

    def advance(s):
        hand_over(s - 1)
        forward(s)

    over(1, segs, advance)
    for i in range(lanes):
        green.put((i,), left[segs - 1, i])
        emit(segs - 1, i, left[segs - 1, i])

    def backward(turn):
        s = segs - 1 - turn

        def settle():
            for i in range(lanes):
                green.put((i,), product(green.get(i), right.get(s, i), alone))
            for i in range(lanes):
                value = left[s, i] + product(outer.get(s, i), green.get(i), alone)
                green.put((i,), value)
                emit(s, i, value)

        if wanted is None:
            settle()
        else:
            pl.when(wanted(s))(settle)

    over(1, segs, backward)


def pieces(target, own, received, at):
    seg, segs, parity = at
    copies = [(own, target.at[seg])]
    for d in range(1, segs):
        source = lax.rem(seg - d + segs, segs)
        copies += parts(received[d - 1], target.at[source], parity)
    return copies


def parts(received, target, parity):
    if len(received) == 1:
        return [(received[0], target)]
    half = target.shape[0] // 2
    return [
        (block, target.at[pl.ds(pl.multiple_of(which * half, half), half), :])
        for block, which in zip(received, (parity, 1 - parity))
    ]


def started(ends, sems):
    copies = [pltpu.make_async_copy(*pair, sems.at[k]) for k, pair in enumerate(ends)]
    for copy in copies:
        copy.start()
    return copies


def wait(copies):
    for copy in copies:
        copy.wait()


def taken(refs, segs, each):
    own, *refs = refs
    return own, [refs[each * k : each * (k + 1)] for k in range(segs - 1)], refs[each * (segs - 1) :]


def choose(index, levels, chosen, count):
    total = jnp.int32(0)
    for sign in (-1, 1):
        for k in range(2):
            source = index[0] + sign * index[2 + k]
            inside = (source >= 0) & (source < count)
            chosen[total] = levels[jnp.clip(source, 0, count - 1)]
            total = total + inside.astype(jnp.int32)
    return total


def in_turns(total, lanes, turn):
    whole = total // lanes
    lax.fori_loop(0, whole, lambda k, _: (turn(k * lanes, lanes), None)[1], None)
    if lanes > 1:
        lax.fori_loop(whole * lanes, total, lambda k, _: (turn(k, 1), None)[1], None)


def first_blocks(segs, count, lanes, index, levels, *refs):
    own, received, (left, onsite, power, poly, row_scale, sems, chosen) = taken(refs, segs, 2)
    seg, parity = index[1], lax.rem(index[0], 2)
    n = onsite.shape[0]

    @pl.when(seg == 0)
    def _():
        wait(started([(own, onsite)], sems))

    for d in range(1, segs):

        @pl.when(seg == d)
        def _():
            wait(started(parts(received[d - 1], onsite, parity), sems))

    total = choose(index, levels, chosen, count)

    def turn(at, width):
        def load(i):
            return onsite[...] + jnp.where(eye_mask(n), chosen[at + i], 0.0)

        def store(i, value):
            left[at + i] = value

        invert([functools.partial(load, i) for i in range(width)], Pair(power), Pair(poly), row_scale, store)

    in_turns(total, lanes, turn)


def by_distance(own, received, seg, segs):
    for d in range(segs):
        yield lax.rem(seg - d + segs, segs), own if d == 0 else received[d - 1][0]


def prepared(own, received, coupling, coupling_t, seg, segs):
    for s, block in by_distance(own, received, seg, segs):

        @pl.when(s > 0)
        def _():
            value = block[...]
            coupling.put((s,), value)
            coupling_t.put((s,), value.T)


def first_round(segs, count, lanes, index, levels, *refs):
    own_matrix, received_matrix, refs = taken(refs, segs, 2)
    own_coupling, received_coupling, refs = taken(refs, segs, 1)
    first, combined, onsite, coupling, coupling_t, left, left_pair, green, right, outer, power, poly, row_scale, sems, chosen = refs
    at = (index[1], segs, lax.rem(index[0], 2))
    copies = started(pieces(onsite, own_matrix, received_matrix, at), sems)
    total = choose(index, levels, chosen, count)
    combined[...] = jnp.zeros_like(combined)
    coupling, coupling_t = Pair(coupling), Pair(coupling_t)
    prepared(own_coupling, received_coupling, coupling, coupling_t, index[1], segs)
    wait(copies)
    n = onsite.shape[1]

    def turn(at, width):
        for i in range(width):
            left[0, i] = first[at + i]

        def matrix(s, i):
            return onsite[s] + jnp.where(eye_mask(n), chosen[at + i], 0.0)

        def emit(s, i, value):
            combined[s] += value

        sweep(
            width, segs, matrix, coupling, coupling_t, left, Pair(left_pair), Pair(green),
            (Pair(right), Pair(outer)), Pair(power), Pair(poly), row_scale, emit, given=True,
        )

    in_turns(total, lanes, turn)


def second_round(segs, index, level, *refs):
    own_matrix, received_matrix, refs = taken(refs, segs, 2)
    own_coupling, received_coupling, refs = taken(refs, segs, 1)
    own_phonon, received_phonon, refs = taken(refs, segs, 1)
    combined, green_out, energy_out, *refs = refs
    onsite, coupling, coupling_t, left, left_pair, green, right, outer, power, poly, row_scale, sems, scattered = refs
    seg = index[1]
    copies = started(pieces(onsite, own_matrix, received_matrix, (seg, segs, lax.rem(index[0], 2))), sems)
    coupling, coupling_t, right, outer = Pair(coupling), Pair(coupling_t), Pair(right), Pair(outer)
    n = onsite.shape[1]
    blocks = list(by_distance(own_phonon, received_phonon, seg, segs))
    for d, (s, block) in enumerate(blocks):
        coupling.put((d,), block[...])
        right.put((d, 0), combined[s])
        outer.put((d, 0), product(coupling.get(d), right.get(d, 0)))
        coupling_t.put((d,), block[...].T)
    for d, (s, block) in enumerate(blocks):
        value = product(outer.get(d, 0), coupling_t.get(d), True)
        scattered[s] = value
        if d == 0:
            energy_out[...] = value
    prepared(own_coupling, received_coupling, coupling, coupling_t, seg, segs)
    wait(copies)

    def matrix(s, i):
        return onsite[s] + jnp.where(eye_mask(n), level[0], 0.0) + scattered[s]

    def emit(s, i, value):
        @pl.when(seg == s)
        def _():
            green_out[...] = value

    sweep(
        1, segs, matrix, coupling, coupling_t, left, Pair(left_pair), Pair(green),
        (right, outer), Pair(power), Pair(poly), row_scale, emit, lambda s: seg <= s,
    )


def pair(n, *lead):
    return pltpu.VMEM((*lead, 2, n, n), BF16)


def full(n, *lead):
    return pltpu.VMEM((*lead, n, n), F32)


def workspace(segs, n, lanes):
    return [
        full(n, segs), pair(n, segs), pair(n, segs), full(n, segs, lanes), pair(n, lanes), pair(n, lanes),
        pair(n, segs, lanes), pair(n, segs, lanes), pair(n, lanes), pair(n, lanes), pltpu.VMEM((lanes, n, 128), F32),
        pltpu.SemaphoreType.DMA((2 * segs,)),
    ]


def held(shapes):
    return sum(4 * math.prod(s.shape) for s in shapes if s.dtype == F32) + sum(2 * math.prod(s.shape) for s in shapes if s.dtype == BF16)


def call(body, out_shape, operands, scratch, flops, copied):
    smem, vmem, anywhere = (pl.BlockSpec(memory_space=m) for m in (pltpu.SMEM, pltpu.VMEM, pl.ANY))
    outs = jax.tree.leaves(out_shape)
    return pl.pallas_call(
        body,
        out_shape=out_shape,
        in_specs=[smem, smem] + [anywhere] * copied + [vmem] * (len(operands) - 2 - copied),
        out_specs=jax.tree.map(lambda _: vmem, out_shape),
        scratch_shapes=scratch,
        compiler_params=pltpu.CompilerParams(vmem_limit_bytes=held(scratch + outs + list(operands[2 + copied :])) + SPARE_BYTES),
        cost_estimate=pl.CostEstimate(flops=flops, bytes_accessed=held(outs), transcendentals=0),
    )(*operands)


def swapped(block, axis, distance):
    size = lax.axis_size(axis)
    return lax.ppermute(block, axis, [(i, (i + distance) % size) for i in range(size)])


def partner(block, axis, bit):
    size = lax.axis_size(axis)
    return lax.ppermute(block, axis, [(i, i ^ bit) for i in range(size)])


def every_level(levels):
    size, bit = lax.axis_size("energy"), 1
    place_of = lax.axis_index("energy")
    while bit < size:
        other = partner(levels, "energy", bit)
        low = place_of & bit == 0
        levels = jnp.where(low, jnp.concatenate([levels, other]), jnp.concatenate([other, levels]))
        bit *= 2
    return levels


def half_of(block):
    half = block.shape[0] // 2
    return lax.dynamic_slice_in_dim(block, lax.axis_index("energy") % 2 * half, half, 0)


def from_others(block):
    received = []
    for d in range(1, lax.axis_size("seg")):
        received.append(swapped(block, "seg", d))
    return received


def with_partner(halves):
    return [part for half in halves for part in (half, partner(half, "energy", 1))]


def shards(onsite, coupling, phonon, levels, offsets):
    return both_rounds(onsite[0], coupling[0], phonon[0], levels, offsets)


def both_rounds(onsite, coupling, phonon, levels, offsets):
    segs, count = lax.axis_size("seg"), lax.axis_size("energy")
    n = onsite.shape[-1]
    energy, seg = lax.axis_index("energy"), lax.axis_index("seg")

    def less_lead(block, rows):
        lead = jnp.matmul(rows, coupling.T, precision=lax.Precision.HIGH) * 0.25
        return block - jnp.where(seg == 0, lead, 0.0)

    matrix_half = less_lead(half_of(onsite), half_of(coupling))
    halves = from_others(matrix_half)
    matrices = with_partner(halves)
    all_levels = every_level(levels)
    matrix = less_lead(onsite, lax.optimization_barrier((coupling, matrix_half))[0])
    couplings = from_others(coupling)
    phonons = from_others(phonon)
    index = jnp.concatenate([jnp.stack([energy, seg]).astype(jnp.int32), offsets])
    lanes = 2 if held(workspace(segs, n, 2)) + (2 * segs + TERMS) * 4 * n * n < VMEM_BYTES else 1
    shape = functools.partial(jax.ShapeDtypeStruct, dtype=F32)
    chosen = pltpu.SMEM((2 * TERMS,), jnp.float32)
    first = call(
        functools.partial(first_blocks, segs, count, lanes),
        shape((TERMS, n, n)),
        [index, all_levels, matrix, *matrices],
        [full(n), pair(n, lanes), pair(n, lanes), pltpu.VMEM((lanes, n, 128), F32), pltpu.SemaphoreType.DMA((2,)), chosen],
        12 * n**3 * TERMS * 3,
        2 * segs - 1,
    )
    combined = call(
        functools.partial(first_round, segs, count, lanes),
        shape((segs, n, n)),
        [index, all_levels, matrix, *matrices, coupling, *couplings, first],
        workspace(segs, n, lanes) + [chosen],
        22 * n**3 * TERMS * 3 * (segs - 1),
        2 * segs - 1,
    )
    green, self_energy = call(
        functools.partial(second_round, segs),
        [shape((n, n))] * 2,
        [index, levels, matrix, *matrices, coupling, *couplings, phonon, *phonons, combined],
        workspace(segs, n, 1) + [full(n, segs)],
        36 * n**3 * 3,
        2 * segs - 1,
    )
    return green[None, None], self_energy[None, None]


def solution(mesh):
    in_specs = (P("seg", None, None), P("seg", None, None), P("seg", None, None), P("energy"), P())
    out_specs = (P("energy", "seg", None, None), P("energy", "seg", None, None))
    return jax.shard_map(shards, mesh=mesh, in_specs=in_specs, out_specs=out_specs, check_vma=False)
```

```python
import functools
import math

import jax
import jax.numpy as jnp
from jax import lax
from jax.experimental import pallas as pl
from jax.experimental.pallas import tpu as pltpu
from jax.sharding import PartitionSpec as P


NS = 4
TERMS = 4
TAIL = 128
VMEM_BYTES = 52 * 2**20
SPARE_BYTES = 8 * 2**20
F32, BF16 = jnp.float32, jnp.bfloat16


def split(x):
    high = x.astype(BF16)
    return high, (x - high.astype(F32)).astype(BF16)


def product(a, b, alone=False):
    rows = a[0].shape[0]
    cut = rows - TAIL if alone else rows
    order = [(which, lo, hi) for lo, hi in ((0, cut), (cut, rows)) if lo < hi for which in ((0, 0), (0, 1), (1, 0))]
    left = jnp.concatenate([a[i][:, lo:hi] for (i, _), lo, hi in order], axis=1)
    right = jnp.concatenate([b[j][lo:hi] for (_, j), lo, hi in order], axis=0)
    parts = [left[:cut], left[cut:]] if alone else [left]
    parts = [jnp.dot(part, right, preferred_element_type=F32) for part in parts]
    return jnp.concatenate(parts, axis=0) if alone else parts[0]


def beside(a, b):
    return tuple(jnp.concatenate([x, y], axis=1) for x, y in zip(a, b))


def joined(a):
    return a[0].astype(F32) + a[1].astype(F32)


def eye_mask(n):
    return lax.broadcasted_iota(jnp.int32, (n, n), 0) == lax.broadcasted_iota(jnp.int32, (n, n), 1)


def diagonal(x, axis):
    n, step = x.shape[0], 128
    mask = eye_mask(step)
    blocks = [
        jnp.sum(jnp.where(mask, x[i : i + step, i : i + step], 0.0), axis=axis, keepdims=True)
        for i in range(0, n, step)
    ]
    return jnp.concatenate(blocks, axis=1 - axis)


def over(low, high, body):
    if high - low == 1:
        body(low)
    elif high > low:
        lax.fori_loop(low, high, lambda s, _: (body(s), None)[1], None)


class Pair:
    def __init__(self, ref):
        self.ref = ref

    def put(self, index, value):
        self.ref[(*index, 0)], self.ref[(*index, 1)] = split(value)

    def get(self, *index):
        return self.ref[(*index, 0)], self.ref[(*index, 1)]


def invert(matrices, power, poly, row_scale, store):
    lanes = range(len(matrices))
    alone = len(matrices) == 1
    for i in lanes:
        x = matrices[i]()
        n = x.shape[0]
        identity = jnp.where(eye_mask(n), 1.0, 0.0)
        residual = identity - x * (1.0 / diagonal(x, 0))
        row_scale[i] = jnp.broadcast_to(1.0 / diagonal(x, 1), (n, 128))
        power.put((i,), residual)
        poly.put((i,), identity + residual)
    for i in lanes:
        e = power.get(i)
        power.put((i,), product(e, e, alone))
    for _ in range(2, NS):
        for i in lanes:
            e, p = power.get(i), poly.get(i)
            both = product(e, beside(e, p), alone)
            n = both.shape[0]
            power.put((i,), both[:, :n])
            poly.put((i,), both[:, n:] + joined(p))
    for i in lanes:
        p = poly.get(i)
        total = product(power.get(i), p, alone) + joined(p)
        n = total.shape[0]
        store(i, total * jnp.concatenate([row_scale[i]] * (n // 128), axis=1))


def sweep(lanes, segs, matrix, coupling, coupling_t, left, left_pair, green, work, power, poly, row_scale, emit, wanted=None, given=False):
    right, outer = work
    alone = lanes == 1

    def forward(s):
        def load(i):
            x = matrix(s, i)
            if not (isinstance(s, int) and s == 0):
                x = x - left[s, i]
            return x

        def store(i, value):
            left[s, i] = value
            left_pair.put((i,), value)

        invert([functools.partial(load, i) for i in range(lanes)], power, poly, row_scale, store)

    def hand_over(s):
        for i in range(lanes):
            outer.put((s, i), product(left_pair.get(i), coupling_t.get(s + 1), alone))
        for i in range(lanes):
            both = product(coupling.get(s + 1), beside(left_pair.get(i), outer.get(s, i)), alone)
            n = both.shape[0]
            right.put((s, i), both[:, :n])
            left[s + 1, i] = both[:, n:]

    if given:
        for i in range(lanes):
            left_pair.put((i,), left[0, i])
    else:
        forward(0)

    def advance(s):
        hand_over(s - 1)
        forward(s)

    over(1, segs, advance)
    for i in range(lanes):
        green.put((i,), left[segs - 1, i])
        emit(segs - 1, i, left[segs - 1, i])

    def backward(turn):
        s = segs - 1 - turn

        def settle():
            for i in range(lanes):
                green.put((i,), product(green.get(i), right.get(s, i), alone))
            for i in range(lanes):
                value = left[s, i] + product(outer.get(s, i), green.get(i), alone)
                green.put((i,), value)
                emit(s, i, value)

        if wanted is None:
            settle()
        else:
            pl.when(wanted(s))(settle)

    over(1, segs, backward)


def pieces(target, own, received, at):
    seg, segs, parity = at
    copies = [(own, target.at[seg])]
    for d in range(1, segs):
        source = lax.rem(seg - d + segs, segs)
        copies += parts(received[d - 1], target.at[source], parity)
    return copies


def parts(received, target, parity):
    if len(received) == 1:
        return [(received[0], target)]
    half = target.shape[0] // 2
    return [
        (block, target.at[pl.ds(pl.multiple_of(which * half, half), half), :])
        for block, which in zip(received, (parity, 1 - parity))
    ]


def started(ends, sems):
    copies = [pltpu.make_async_copy(*pair, sems.at[k]) for k, pair in enumerate(ends)]
    for copy in copies:
        copy.start()
    return copies


def wait(copies):
    for copy in copies:
        copy.wait()


def taken(refs, segs, each):
    own, *refs = refs
    return own, [refs[each * k : each * (k + 1)] for k in range(segs - 1)], refs[each * (segs - 1) :]


def choose(index, levels, chosen, count):
    total = jnp.int32(0)
    for sign in (-1, 1):
        for k in range(2):
            source = index[0] + sign * index[2 + k]
            inside = (source >= 0) & (source < count)
            chosen[total] = levels[jnp.clip(source, 0, count - 1)]
            total = total + inside.astype(jnp.int32)
    return total


def in_turns(total, lanes, turn):
    whole = total // lanes
    lax.fori_loop(0, whole, lambda k, _: (turn(k * lanes, lanes), None)[1], None)
    if lanes > 1:
        lax.fori_loop(whole * lanes, total, lambda k, _: (turn(k, 1), None)[1], None)


def first_blocks(segs, count, lanes, index, levels, *refs):
    own, received, (left, onsite, power, poly, row_scale, sems, chosen) = taken(refs, segs, 2)
    seg, parity = index[1], lax.rem(index[0], 2)
    n = onsite.shape[0]

    @pl.when(seg == 0)
    def _():
        wait(started([(own, onsite)], sems))

    for d in range(1, segs):

        @pl.when(seg == d)
        def _():
            wait(started(parts(received[d - 1], onsite, parity), sems))

    total = choose(index, levels, chosen, count)

    def turn(at, width):
        def load(i):
            return onsite[...] + jnp.where(eye_mask(n), chosen[at + i], 0.0)

        def store(i, value):
            left[at + i] = value

        invert([functools.partial(load, i) for i in range(width)], Pair(power), Pair(poly), row_scale, store)

    in_turns(total, lanes, turn)


def by_distance(own, received, seg, segs):
    for d in range(segs):
        yield lax.rem(seg - d + segs, segs), own if d == 0 else received[d - 1][0]


def prepared(own, received, coupling, coupling_t, seg, segs):
    for s, block in by_distance(own, received, seg, segs):
        value = block[...]
        coupling.put((s,), value)
        coupling_t.put((s,), value.T)


def first_round(segs, count, lanes, index, levels, *refs):
    own_matrix, received_matrix, refs = taken(refs, segs, 2)
    own_coupling, received_coupling, refs = taken(refs, segs, 1)
    first, combined, onsite, coupling, coupling_t, left, left_pair, green, right, outer, power, poly, row_scale, sems, chosen = refs
    at = (index[1], segs, lax.rem(index[0], 2))
    copies = started(pieces(onsite, own_matrix, received_matrix, at), sems)
    total = choose(index, levels, chosen, count)
    combined[...] = jnp.zeros_like(combined)
    coupling, coupling_t = Pair(coupling), Pair(coupling_t)
    prepared(own_coupling, received_coupling, coupling, coupling_t, index[1], segs)
    wait(copies)
    n = onsite.shape[1]

    def turn(at, width):
        for i in range(width):
            left[0, i] = first[at + i]

        def matrix(s, i):
            return onsite[s] + jnp.where(eye_mask(n), chosen[at + i], 0.0)

        def emit(s, i, value):
            combined[s] += value

        sweep(
            width, segs, matrix, coupling, coupling_t, left, Pair(left_pair), Pair(green),
            (Pair(right), Pair(outer)), Pair(power), Pair(poly), row_scale, emit, given=True,
        )

    in_turns(total, lanes, turn)


def second_round(segs, index, level, *refs):
    own_matrix, received_matrix, refs = taken(refs, segs, 2)
    own_coupling, received_coupling, refs = taken(refs, segs, 1)
    own_phonon, received_phonon, refs = taken(refs, segs, 1)
    combined, green_out, energy_out, *refs = refs
    onsite, coupling, coupling_t, left, left_pair, green, right, outer, power, poly, row_scale, sems, scattered, phonon, phonon_t = refs
    seg = index[1]
    copies = started(pieces(onsite, own_matrix, received_matrix, (seg, segs, lax.rem(index[0], 2))), sems)
    coupling, coupling_t, right, outer = Pair(coupling), Pair(coupling_t), Pair(right), Pair(outer)
    phonon, phonon_t = Pair(phonon), Pair(phonon_t)
    n = onsite.shape[1]
    blocks = list(by_distance(own_phonon, received_phonon, seg, segs))
    for d, (s, block) in enumerate(blocks):
        phonon.put((d,), block[...])
        right.put((d, 0), combined[s])
        outer.put((d, 0), product(phonon.get(d), right.get(d, 0)))
        phonon_t.put((d,), block[...].T)
    prepared(own_coupling, received_coupling, coupling, coupling_t, seg, segs)
    wait(copies)
    for d, (s, block) in enumerate(blocks):
        value = product(outer.get(d, 0), phonon_t.get(d), True)
        scattered[s] = value
        if d == 0:
            energy_out[...] = value

    def matrix(s, i):
        return onsite[s] + jnp.where(eye_mask(n), level[0], 0.0) + scattered[s]

    def emit(s, i, value):
        @pl.when(seg == s)
        def _():
            green_out[...] = value

    sweep(
        1, segs, matrix, coupling, coupling_t, left, Pair(left_pair), Pair(green),
        (right, outer), Pair(power), Pair(poly), row_scale, emit, lambda s: seg <= s,
    )


def pair(n, *lead):
    return pltpu.VMEM((*lead, 2, n, n), BF16)


def full(n, *lead):
    return pltpu.VMEM((*lead, n, n), F32)


def workspace(segs, n, lanes):
    return [
        full(n, segs), pair(n, segs), pair(n, segs), full(n, segs, lanes), pair(n, lanes), pair(n, lanes),
        pair(n, segs, lanes), pair(n, segs, lanes), pair(n, lanes), pair(n, lanes), pltpu.VMEM((lanes, n, 128), F32),
        pltpu.SemaphoreType.DMA((2 * segs,)),
    ]


def held(shapes):
    return sum(4 * math.prod(s.shape) for s in shapes if s.dtype == F32) + sum(2 * math.prod(s.shape) for s in shapes if s.dtype == BF16)


def call(body, out_shape, operands, scratch, flops, copied):
    smem, vmem, anywhere = (pl.BlockSpec(memory_space=m) for m in (pltpu.SMEM, pltpu.VMEM, pl.ANY))
    outs = jax.tree.leaves(out_shape)
    return pl.pallas_call(
        body,
        out_shape=out_shape,
        in_specs=[smem, smem] + [anywhere] * copied + [vmem] * (len(operands) - 2 - copied),
        out_specs=jax.tree.map(lambda _: vmem, out_shape),
        scratch_shapes=scratch,
        compiler_params=pltpu.CompilerParams(vmem_limit_bytes=held(scratch + outs + list(operands[2 + copied :])) + SPARE_BYTES),
        cost_estimate=pl.CostEstimate(flops=flops, bytes_accessed=held(outs), transcendentals=0),
    )(*operands)


def swapped(block, axis, distance):
    size = lax.axis_size(axis)
    return lax.ppermute(block, axis, [(i, (i + distance) % size) for i in range(size)])


def partner(block, axis, bit):
    size = lax.axis_size(axis)
    return lax.ppermute(block, axis, [(i, i ^ bit) for i in range(size)])


def every_level(levels):
    size, bit = lax.axis_size("energy"), 1
    place_of = lax.axis_index("energy")
    while bit < size:
        other = partner(levels, "energy", bit)
        low = place_of & bit == 0
        levels = jnp.where(low, jnp.concatenate([levels, other]), jnp.concatenate([other, levels]))
        bit *= 2
    return levels


def half_of(block):
    half = block.shape[0] // 2
    return lax.dynamic_slice_in_dim(block, lax.axis_index("energy") % 2 * half, half, 0)


def from_others(block):
    received = []
    for d in range(1, lax.axis_size("seg")):
        received.append(swapped(block, "seg", d))
    return received


def with_partner(halves):
    return [part for half in halves for part in (half, partner(half, "energy", 1))]


def shards(onsite, coupling, phonon, levels, offsets):
    return both_rounds(onsite[0], coupling[0], phonon[0], levels, offsets)


def both_rounds(onsite, coupling, phonon, levels, offsets):
    segs, count = lax.axis_size("seg"), lax.axis_size("energy")
    n = onsite.shape[-1]
    energy, seg = lax.axis_index("energy"), lax.axis_index("seg")

    def less_lead(block, rows):
        lead = jnp.matmul(rows, coupling.T, precision=lax.Precision.HIGH) * 0.25
        return block - jnp.where(seg == 0, lead, 0.0)

    matrix_half = less_lead(half_of(onsite), half_of(coupling))
    halves = from_others(matrix_half)
    matrices = with_partner(halves)
    all_levels = every_level(levels)
    matrix = less_lead(onsite, lax.optimization_barrier((coupling, matrix_half))[0])
    couplings = from_others(coupling)
    phonons = from_others(phonon)
    index = jnp.concatenate([jnp.stack([energy, seg]).astype(jnp.int32), offsets])
    lanes = 2 if held(workspace(segs, n, 2)) + (2 * segs + TERMS) * 4 * n * n < VMEM_BYTES else 1
    shape = functools.partial(jax.ShapeDtypeStruct, dtype=F32)
    chosen = pltpu.SMEM((2 * TERMS,), jnp.float32)
    first = call(
        functools.partial(first_blocks, segs, count, lanes),
        shape((TERMS, n, n)),
        [index, all_levels, matrix, *matrices],
        [full(n), pair(n, lanes), pair(n, lanes), pltpu.VMEM((lanes, n, 128), F32), pltpu.SemaphoreType.DMA((2,)), chosen],
        12 * n**3 * TERMS * 3,
        2 * segs - 1,
    )
    combined = call(
        functools.partial(first_round, segs, count, lanes),
        shape((segs, n, n)),
        [index, all_levels, matrix, *matrices, coupling, *couplings, first],
        workspace(segs, n, lanes) + [chosen],
        22 * n**3 * TERMS * 3 * (segs - 1),
        2 * segs - 1,
    )
    green, self_energy = call(
        functools.partial(second_round, segs),
        [shape((n, n))] * 2,
        [index, levels, matrix, *matrices, coupling, *couplings, phonon, *phonons, combined],
        workspace(segs, n, 1) + [full(n, segs), pair(n, segs), pair(n, segs)],
        36 * n**3 * 3,
        2 * segs - 1,
    )
    return green[None, None], self_energy[None, None]


def solution(mesh):
    in_specs = (P("seg", None, None), P("seg", None, None), P("seg", None, None), P("energy"), P())
    out_specs = (P("energy", "seg", None, None), P("energy", "seg", None, None))
    return jax.shard_map(shards, mesh=mesh, in_specs=in_specs, out_specs=out_specs, check_vma=False)
```
